32 devices in a mesh: ty: 4 (over x, core), tx: 8 (over z, y).
Axes of the slice: x: 2, y: 2, z: 4, core: 2. Of those that a mesh axis runs over, the one named last changes fastest.
Arguments:
- exposures: float32 [256, 128, 128], P(('ty', 'tx')), may hold values from -70 to 70
- point_spread: float32 [256, 31, 31], P(('ty', 'tx')), may hold values from 0.0001 to 1
- warp_steps: int32 [256, 2], P(('ty', 'tx')), may hold values from 0 to 3
- column: int32 [256, 1], P(('ty', 'tx')), may hold values from 0 to 7; in each aligned block of 8 rows (0 to 7, 8 to 15, ...) at most 2 rows name the same one
- block_cell: int32 [256], P(('ty', 'tx')), may hold values from 0 to 15
Outputs:
- solution: float32 [2048, 4096], P('ty', 'tx')
- residual: float32 [2048, 4096], P('ty', 'tx')
The draws below stay inside these ranges and needn't reach their ends.
Inputs may be any that keep to these rules, and one draw needn't show every extreme that they name: `column`: among the 8 frame blocks of one device (aligned blocks of 8 rows) no value occurs more than 2 times, and in some such block one value occurs exactly 2 times.
All inputs are finite; a program needn't handle non-finite values.
Results may differ from the reference program's by a relative error of at most 0.0042.
Values may be sent and summed in bfloat16 or wider, within the bound.
A program may use at most 192 MiB of HBM per device.

```python
import math
import jax
import jax.numpy as jnp
import numpy as np
from jax import lax

TILE = 512
FB_DEV = 8
BLOCK = 128
PSF = 31
SUB = 4
ITERS = 2
TAPS = 32
HALO = 16
WIN = 160
CELLS = 16
CAP = 2
FRAMES_ROW = 64
FRAMES = 256
NY = 2048
NX = 4096
N_TX = 8


def draw_exposures(key, part):
    position = jnp.arange(FRAMES, dtype=jnp.float32) / max(FRAMES - 1, 1)
    scales = 1.0 + 2.0 * position
    noise_field = jnp.clip(jax.random.normal(jax.random.fold_in(key, 17), (FRAMES, BLOCK, BLOCK), jnp.float32), -6.0, 6.0)
    return noise_field * scales[:, None, None]


def plant(values, own_key, smallest, high):
    spot = [jax.random.randint(jax.random.fold_in(own_key, axis), (), 0, length) for axis, length in enumerate(values.shape)]
    longest = values.shape.index(max(values.shape))
    next_to = spot[:longest] + [(spot[longest] + 1) % values.shape[longest]] + spot[longest + 1:]
    return values.at[tuple(spot)].set(smallest).at[tuple(next_to)].set(high)


def shard_levels(rng, shape, shards, least, top_value):
    level, own = 1.0, jax.random.fold_in(rng, 6)
    for dim, blocks in shards:
        steps = jnp.exp(jax.random.uniform(jax.random.fold_in(own, dim), (blocks,), jnp.float32, least / len(shards), top_value / len(shards)))
        level = level * jnp.repeat(steps, shape[dim] // blocks).reshape([-1 if axis == dim else 1 for axis in range(len(shape))])
    return level


def assign_block(key, own, number, rows, number_of, top, most, lean):
    order = jax.random.permutation(key, number_of)
    crowded, common = shares(number_of, rows * top, most, lean, True), shares(number_of, rows * top, most, lean, False)
    places = jnp.arange(number_of)

    def named(lengths, rotation):
        used = int((lengths > 0).sum())
        fixed = max(1, used // 4)
        moved = fixed + (places - fixed + rotation * (used - fixed)) % max(1, number_of - fixed)
        return jnp.zeros((number_of,), jnp.int32).at[order[jnp.where(places < fixed, places, moved)]].set(jnp.asarray(lengths, jnp.int32))

    lengths = jnp.where(number % 4 == 0, named(crowded, number // 4), named(common, number - number // 4 - 1))
    mixed = jax.random.permutation(jax.random.fold_in(own, 3), number_of)
    giver, receiver = mixed[0:number_of // 2 * 2:2], mixed[1:number_of // 2 * 2:2]
    slack = jnp.minimum(lengths[giver] - 1, most - lengths[receiver]) // 2
    slack = jnp.where((giver == order[0]) | (receiver == order[0]) | (lengths[receiver] == 0), 0, jnp.maximum(slack, 0))
    moved = jax.random.randint(jax.random.fold_in(own, 4), (number_of // 2,), 0, 1 << 20) % (slack + 1)
    lengths = lengths.at[giver].add(-moved).at[receiver].add(moved)
    members = jnp.searchsorted(jnp.cumsum(lengths), jnp.arange(rows * top), side="right").astype(jnp.int32)
    table = members.reshape(top, rows).T
    table = table[jax.random.permutation(jax.random.fold_in(own, 1), rows)]
    rotation = jax.random.randint(jax.random.fold_in(own, 2), (rows, 1), 0, top)
    return jnp.take_along_axis(table, (jnp.arange(top)[None, :] + rotation) % top, axis=1)


def shares(number_of, total, bound, skew, full):
    weights = [(1 << 20) // math.isqrt(rank ** skew) + 1 for rank in range(1, number_of + 1)]
    largest = bound if full else min(bound, max(-(-total // number_of), total * weights[0] // sum(weights)))
    least = 1 if total - largest >= number_of - 1 else 0
    counts, spare = [largest] + [least] * (number_of - 1), total - largest - least * (number_of - 1)
    while spare > 0:
        candidates = [i for i in range(1, number_of) if counts[i] < largest] or [i for i in range(1, number_of) if counts[i] < bound]
        mass, left = sum([weights[i] for i in candidates]), spare
        for i in candidates:
            extra = min(bound - counts[i], max(1, left * weights[i] // mass), spare)
            counts[i] = counts[i] + extra
            spare = spare - extra
    return np.array(counts)


def setup_inputs(seed: int = 0) -> dict:
    arg_keys = jax.random.split(jax.random.key(seed), 6)
    exposures = draw_exposures(jax.random.fold_in(arg_keys[5], 71), 0)
    point_spread = jnp.clip(jnp.exp(math.log(1.0) - 9.2103404 * jax.random.uniform(arg_keys[1], (FRAMES, PSF, PSF), jnp.float32) ** shard_levels(arg_keys[1], (FRAMES, PSF, PSF), ((0, 32),), -0.2, 0.2)), 0.0001, 1.0)
    warp_steps = plant(jax.random.randint(arg_keys[2], (FRAMES, 2), 0, SUB), jax.random.fold_in(arg_keys[2], 1), 0, SUB - 1).astype(jnp.int32)
    column_keys = jax.random.split(jax.random.fold_in(arg_keys[3], 1), FRAMES // FB_DEV)
    column_turns = jax.random.permutation(jax.random.fold_in(arg_keys[3], 3), FRAMES // FB_DEV)
    column = jax.vmap(lambda own, number: assign_block(jax.random.fold_in(arg_keys[3], 2), own, number, FB_DEV, N_TX, 1, CAP, 2))(column_keys, column_turns).reshape((FRAMES, 1))
    block_cell = plant(jax.random.randint(arg_keys[4], (FRAMES,), 0, CELLS), jax.random.fold_in(arg_keys[4], 1), 0, CELLS - 1).astype(jnp.int32)
    return dict(exposures=exposures, point_spread=point_spread, warp_steps=warp_steps, column=column, block_cell=block_cell)


damping = 0.05


def make_kernels(point_spread, warp_steps):
    tap_count = point_spread.shape[-1] + 1
    totals = jnp.sum(point_spread, axis=(1, 2), keepdims=True)
    padded = jnp.pad(point_spread / totals, ((0, 0), (0, 1), (0, 1)))
    row_frac = (warp_steps[:, 0].astype(jnp.float32) / SUB)[:, None, None]
    col_frac = (warp_steps[:, 1].astype(jnp.float32) / SUB)[:, None, None]
    shifted = jnp.pad(padded, ((0, 0), (0, 0), (1, 0)))[:, :, :tap_count]
    blended = (1.0 - col_frac) * padded + col_frac * shifted
    lowered = jnp.pad(blended, ((0, 0), (1, 0), (0, 0)))[:, :tap_count, :]
    kernel = (1.0 - row_frac) * blended + row_frac * lowered
    return lax.optimization_barrier(kernel.astype(jnp.bfloat16)).astype(jnp.float32)


def rounded(values):
    return lax.optimization_barrier(values.astype(jnp.bfloat16)).astype(jnp.float32)


def window_anchors(column, block_cell):
    frame_index = jnp.arange(FRAMES, dtype=jnp.int32)
    per_row = TILE // BLOCK
    top_rows = (frame_index // FRAMES_ROW) * TILE + (block_cell.astype(jnp.int32) // per_row) * BLOCK
    left_cols = column[:, 0].astype(jnp.int32) * TILE + (block_cell.astype(jnp.int32) % per_row) * BLOCK
    return top_rows.astype(jnp.int32), left_cols.astype(jnp.int32)


def tap_table():
    taps_index = jnp.arange(TAPS)[:, None, None]
    positions = jnp.arange(WIN)[:, None]
    columns = jnp.arange(BLOCK)[None, :]
    table = jnp.where(positions - columns == taps_index, 1.0, 0.0).astype(jnp.float32)
    return table.reshape(TAPS, WIN * BLOCK)


def frame_bands(kernel_one, table):
    return jnp.dot(kernel_one, table, precision=lax.Precision.HIGHEST).reshape(TAPS, WIN, BLOCK)


def grouped(arrays):
    return tuple(member.reshape((FRAMES // FB_DEV, FB_DEV) + member.shape[1:]) for member in arrays)


def forward_all(field, kernels, top_rows, left_cols, table):
    padded = jnp.pad(field, HALO)

    def one_frame(kernel_one, top_row, left_col):
        framed = lax.dynamic_slice(padded, (top_row, left_col), (WIN, WIN))
        bands = frame_bands(kernel_one, table)
        stacked = jnp.stack([framed[offset:offset + BLOCK] for offset in range(TAPS)])
        return jnp.einsum('ayp,apx->yx', stacked, bands, precision=lax.Precision.HIGHEST)

    def one_group(operands):
        return jax.vmap(one_frame)(operands[0], operands[1], operands[2])

    result = lax.map(one_group, grouped((kernels, top_rows, left_cols)))
    return result.reshape(FRAMES, BLOCK, BLOCK)


def adjoint_all(images, kernels, top_rows, left_cols, table):
    def one_frame(frame_image, kernel_one):
        bands = frame_bands(kernel_one, table)
        spread = jnp.einsum('yx,apx->ayp', frame_image, bands, precision=lax.Precision.HIGHEST)
        summed = jnp.zeros((WIN, WIN), spread.dtype)
        for offset in range(TAPS):
            summed = summed + jnp.pad(spread[offset], ((offset, WIN - BLOCK - offset), (0, 0)))
        return summed

    def one_group(operands):
        return jax.vmap(one_frame)(operands[0], operands[1])

    patches = lax.map(one_group, grouped((images, kernels))).reshape(FRAMES, WIN, WIN)
    initial = jnp.zeros((NY + 2 * HALO, NX + 2 * HALO), patches.dtype)

    def place(slot_number, accumulated):
        current = lax.dynamic_slice(accumulated, (top_rows[slot_number], left_cols[slot_number]), (WIN, WIN))
        return lax.dynamic_update_slice(accumulated, current + patches[slot_number], (top_rows[slot_number], left_cols[slot_number]))

    accumulated = lax.fori_loop(0, FRAMES, place, initial)
    return accumulated[HALO:HALO + NY, HALO:HALO + NX]


def reference(exposures, point_spread, warp_steps, column, block_cell):
    kernels = make_kernels(point_spread, warp_steps)
    table = tap_table()
    top_rows, left_cols = window_anchors(column, block_cell)
    right_side = adjoint_all(rounded(exposures), kernels, top_rows, left_cols, table)
    solution = jnp.zeros_like(right_side)
    residual = right_side
    direction = right_side
    norm_now = jnp.sum(residual * residual)
    for iteration in range(ITERS):
        modelled = forward_all(rounded(direction), kernels, top_rows, left_cols, table)
        applied = adjoint_all(rounded(modelled), kernels, top_rows, left_cols, table) + damping * direction
        step_size = norm_now / jnp.sum(direction * applied)
        solution = solution + step_size * direction
        residual = residual - step_size * applied
        if iteration + 1 < ITERS:
            norm_next = jnp.sum(residual * residual)
            direction = residual + (norm_next / norm_now) * direction
            norm_now = norm_next
    return solution, residual
```

```python
import functools

import jax
import jax.numpy as jnp
from jax import lax
from jax.experimental import pallas as pl
from jax.experimental.pallas import tpu as pltpu
from jax.sharding import PartitionSpec as P

TILE = 512
SUB = 4
ITERS = 2
GROUP = 32
LANES = 128

damping = 0.05


def make_kernels(point_spread, warp_steps):
    tap_count = point_spread.shape[-1] + 1
    totals = jnp.sum(point_spread, axis=(1, 2), keepdims=True)
    padded = jnp.pad(point_spread / totals, ((0, 0), (0, 1), (0, 1)))
    row_frac = (warp_steps[:, 0].astype(jnp.float32) / SUB)[:, None, None]
    col_frac = (warp_steps[:, 1].astype(jnp.float32) / SUB)[:, None, None]
    shifted = jnp.pad(padded, ((0, 0), (0, 0), (1, 0)))[:, :, :tap_count]
    blended = (1.0 - col_frac) * padded + col_frac * shifted
    lowered = jnp.pad(blended, ((0, 0), (1, 0), (0, 0)))[:, :tap_count, :]
    return ((1.0 - row_frac) * blended + row_frac * lowered).astype(jnp.bfloat16)


def turn(value, shift, axis):
    size = value.shape[axis]
    shift = shift % size
    return value if shift == 0 else pltpu.roll(value, shift, axis)


def lane_group(shape, width):
    return lax.broadcasted_iota(jnp.int32, shape, 1) // width


def pick_groups(groups, parts):
    value = parts[-1]
    for number in range(len(parts) - 2, -1, -1):
        value = jnp.where(groups == number, parts[number], value)
    return value


def toeplitz(rows):
    tiles = []
    for j in range(8):
        halves = []
        for half in range(2):
            spread = jnp.broadcast_to(rows[2 * j + half : 2 * j + half + 1], (GROUP, LANES))
            halves.append(pltpu.roll(spread, 0, 1, stride=1, stride_axis=0))
        tiles.append(jnp.concatenate(halves, axis=1))
    return jnp.concatenate(tiles, axis=0).astype(jnp.bfloat16)


def blur(left, right, matrix):
    groups = lane_group(left.shape, GROUP)
    low = groups < 2
    by32, by64, by96 = turn(left, 32, 1), turn(left, 64, 1), turn(left, 96, 1)
    end32, end96 = turn(right, 32, 1), turn(right, 96, 1)
    framed = [
        jnp.where(low, left, by64),
        jnp.where(low, by96, by32),
        jnp.where(low, by64, left),
        pick_groups(groups, [by32, end32, by96, end96]),
    ]
    summed = []
    for part in framed:
        first = jnp.where(low, part, turn(part, -1, 0))
        stacked = jnp.concatenate([first, turn(first, -2, 0)], axis=1).astype(jnp.bfloat16)
        product = lax.dot_general(
            stacked, matrix, (((1,), (1,)), ((), ())), preferred_element_type=jnp.float32
        )
        joined = product[:, :LANES] + turn(product[:, LANES:], -16, 0)
        summed.append(pick_groups(groups, [turn(joined, -4 * j, 0) for j in range(4)]))
    total = pick_groups(groups, summed)
    for step in range(1, 4):
        chosen = pick_groups(groups, [summed[(j + step) % 4] for j in range(4)])
        total = total + turn(chosen, 32 * step, 1)
    return total


def blur_back(image, matrix):
    groups = lane_group(image.shape, GROUP)
    low = groups < 2
    turned = [turn(image, 32 * step, 1) for step in range(4)]
    folded = []
    for h in range(4):
        spread = pick_groups(groups, [turned[(j - h) % 4] for j in range(4)])
        first = pick_groups(groups, [turn(spread, 4 * j, 0) for j in range(4)])
        stacked = jnp.concatenate([first, turn(first, 16, 0)], axis=1).astype(jnp.bfloat16)
        product = jnp.dot(stacked, matrix, preferred_element_type=jnp.float32)
        joined = product[:, :LANES] + turn(product[:, LANES:], 2, 0)
        shifted = jnp.where(low, joined, turn(joined, 1, 0))
        folded.append(shifted + turn(shifted, 64, 1))
    one, three = turn(folded[1], 32, 1), turn(folded[3], 32, 1)
    zero = jnp.zeros_like(one)
    left = jnp.where(low, folded[0], folded[2]) + pick_groups(groups, [zero, one, one, three])
    right = jnp.where(groups == 0, three, 0.0)
    return left, right


def place(total_ref, cell, per_row, block, patch):
    left, right = patch
    rows = pl.ds(pl.multiple_of(cell // per_row * block, block), left.shape[0])
    start = pl.multiple_of(cell % per_row * block, block)
    total_ref[rows, pl.ds(start, block)] += left
    total_ref[rows, pl.ds(pl.multiple_of(start + block, block), block)] += right


def pack_kernel(count, source_ref, tag_ref, exposures_ref, taps_ref, out_ref):
    block = exposures_ref.shape[1]

    @pl.loop(0, count)
    def _(slot):
        origin = source_ref[slot]
        out_ref[slot, :block, :] = exposures_ref[origin].astype(jnp.bfloat16)
        out_ref[slot, block : block + 16, :] = taps_ref[origin]
        out_ref[slot, block + 16 :, :] = jnp.full((16, LANES), tag_ref[slot], jnp.float32).astype(
            jnp.bfloat16
        )


def first_kernel(count, per_row, block, cell_ref, frames_ref, total_ref, matrix_ref):
    total_ref[...] = jnp.zeros_like(total_ref)

    @pl.loop(0, count)
    def _(slot):
        cell = cell_ref[slot]

        @pl.when(cell >= 0)
        def _():
            frame = frames_ref[slot]
            matrix = toeplitz(frame[block : block + 16].astype(jnp.float32))
            matrix_ref[slot] = matrix
            image = frame[:block].astype(jnp.float32)
            image = jnp.concatenate([image, jnp.zeros((GROUP, LANES), jnp.float32)], axis=0)
            place(total_ref, cell, per_row, block, blur_back(image, matrix))


def normal_kernel(count, per_row, block, cell_ref, field_ref, matrix_ref, total_ref):
    total_ref[...] = jnp.zeros_like(total_ref)
    window = block + GROUP

    @pl.loop(0, count)
    def _(slot):
        cell = cell_ref[slot]

        @pl.when(cell >= 0)
        def _():
            matrix = matrix_ref[slot]
            rows = pl.ds(pl.multiple_of(cell // per_row * block, block), window)
            start = pl.multiple_of(cell % per_row * block, block)
            left = field_ref[rows, pl.ds(start, block)].astype(jnp.float32)
            right = field_ref[rows, pl.ds(pl.multiple_of(start + block, block), block)].astype(
                jnp.float32
            )
            modelled = blur(left, right, matrix).astype(jnp.bfloat16).astype(jnp.float32)
            inside = lax.broadcasted_iota(jnp.int32, modelled.shape, 0) < block
            image = jnp.where(inside, modelled, 0.0)
            place(total_ref, cell, per_row, block, blur_back(image, matrix))


def vmem():
    return pl.BlockSpec(memory_space=pltpu.VMEM)


def smem():
    return pl.BlockSpec(memory_space=pltpu.SMEM)


def share_edges(value, axis, dim, width):
    size, length = lax.axis_size(axis), value.shape[dim]
    position = lax.axis_index(axis)
    up = [(i, i + 1) for i in range(size - 1)]
    down = [(j, i) for i, j in up]
    first = lax.slice_in_dim(value, 0, 2 * width, axis=dim)
    middle = lax.slice_in_dim(value, 2 * width, length - 2 * width, axis=dim)
    last = lax.slice_in_dim(value, length - 2 * width, length, axis=dim)
    before = lax.ppermute(last, axis, up)
    after = lax.ppermute(first, axis, down)
    index = lax.broadcasted_iota(jnp.int32, first.shape, dim)
    first = jnp.where((position > 0) | (index >= width), first + before, 0.0)
    last = jnp.where((position < size - 1) | (index < width), last + after, 0.0)
    return jnp.concatenate([first, middle, last], axis=dim)


def body(exposures, point_spread, warp_steps, column, block_cell):
    frame_count, block = exposures.shape[:2]
    tap_count = point_spread.shape[1] + 1
    margin = tap_count // 2
    tx_size = lax.axis_size("tx")
    capacity = max(2, 2 * frame_count // tx_size)
    slot_count = tx_size * capacity
    per_row = TILE // block
    extent = TILE + 2 * margin
    wide = TILE + block
    taps = make_kernels(point_spread, warp_steps)
    taps = jnp.pad(taps, ((0, 0), (0, 0), (0, 64 - tap_count))).reshape(frame_count, 16, LANES)

    target = column[:, 0]
    earlier = jnp.arange(frame_count)[:, None] > jnp.arange(frame_count)[None, :]
    matching = target[:, None] == target[None, :]
    standing = jnp.sum(jnp.where(earlier & matching, 1, 0), axis=1)
    slot_index = target * capacity + standing
    chosen = slot_index[None, :] == jnp.arange(slot_count)[:, None]
    source = jnp.sum(jnp.where(chosen, jnp.arange(frame_count)[None, :], 0), axis=1).astype(jnp.int32)
    tag = jnp.sum(jnp.where(chosen, block_cell[None, :] + 1, 0), axis=1).astype(jnp.float32)

    packed = pl.pallas_call(
        functools.partial(pack_kernel, slot_count),
        out_shape=jax.ShapeDtypeStruct((slot_count, block + 32, LANES), jnp.bfloat16),
        in_specs=[smem(), smem(), vmem(), vmem()],
        out_specs=vmem(),
        name="pack",
    )(source, tag, exposures, taps)
    frames = lax.all_to_all(packed, "tx", split_axis=0, concat_axis=0, tiled=True)
    cells = frames[:, block + 16, 0].astype(jnp.int32) - 1

    total, matrices = pl.pallas_call(
        functools.partial(first_kernel, slot_count, per_row, block),
        out_shape=(
            jax.ShapeDtypeStruct((extent, wide), jnp.float32),
            jax.ShapeDtypeStruct((slot_count, 256, 256), jnp.bfloat16),
        ),
        in_specs=[smem(), vmem()],
        out_specs=(vmem(), vmem()),
        name="first_adjoint",
    )(cells, frames)

    def finish(total):
        value = share_edges(total[:, :extent], "ty", 0, margin)
        return share_edges(value, "tx", 1, margin)

    def inner(value):
        return value[margin : margin + TILE, margin : margin + TILE]

    def products(pairs):
        return tuple(jnp.sum(inner(left * right)) for left, right in pairs)

    residual = finish(total)
    direction = residual
    solution = jnp.zeros((TILE, TILE), jnp.float32)
    norm_now = None
    for iteration in range(ITERS):
        field = jnp.pad(direction.astype(jnp.bfloat16), ((0, 0), (0, wide - extent)))
        total = pl.pallas_call(
            functools.partial(normal_kernel, slot_count, per_row, block),
            out_shape=jax.ShapeDtypeStruct((extent, wide), jnp.float32),
            in_specs=[smem(), vmem(), vmem()],
            out_specs=vmem(),
            name="normal",
        )(cells, field, matrices)
        applied = finish(total) + damping * direction
        last = iteration + 1 == ITERS
        pairs = [(direction, applied)]
        if not last:
            pairs = pairs + [(residual, applied), (applied, applied)]
        if norm_now is None:
            pairs = pairs + [(residual, residual)]
        sums = lax.psum(jnp.stack(products(pairs)), ("ty", "tx"))
        if norm_now is None:
            norm_now = sums[-1]
        step_size = norm_now / sums[0]
        solution = solution + step_size * inner(direction)
        residual = residual - step_size * applied
        if not last:
            norm_next = norm_now - 2.0 * step_size * sums[1] + step_size * step_size * sums[2]
            direction = residual + norm_next / norm_now * direction
            norm_now = norm_next
    return solution, inner(residual)


def solution(mesh):
    placed = (
        P(("ty", "tx"), None, None),
        P(("ty", "tx"), None, None),
        P(("ty", "tx"), None),
        P(("ty", "tx"), None),
        P(("ty", "tx")),
    )
    return jax.shard_map(
        body, mesh=mesh, in_specs=placed, out_specs=(P("ty", "tx"), P("ty", "tx")), check_vma=False
    )
```

```python
import functools

import jax
import jax.numpy as jnp
from jax import lax
from jax.experimental import pallas as pl
from jax.experimental.pallas import tpu as pltpu
from jax.sharding import PartitionSpec as P

TILE = 512
SUB = 4
ITERS = 2
GROUP = 32
LANES = 128

damping = 0.05


def make_kernels(point_spread, warp_steps):
    tap_count = point_spread.shape[-1] + 1
    totals = jnp.sum(point_spread, axis=(1, 2), keepdims=True)
    padded = jnp.pad(point_spread / totals, ((0, 0), (0, 1), (0, 1)))
    row_frac = (warp_steps[:, 0].astype(jnp.float32) / SUB)[:, None, None]
    col_frac = (warp_steps[:, 1].astype(jnp.float32) / SUB)[:, None, None]
    shifted = jnp.pad(padded, ((0, 0), (0, 0), (1, 0)))[:, :, :tap_count]
    blended = (1.0 - col_frac) * padded + col_frac * shifted
    lowered = jnp.pad(blended, ((0, 0), (1, 0), (0, 0)))[:, :tap_count, :]
    return ((1.0 - row_frac) * blended + row_frac * lowered).astype(jnp.bfloat16)


def turn(value, shift, axis):
    size = value.shape[axis]
    shift = shift % size
    return value if shift == 0 else pltpu.roll(value, shift, axis)


def lane_group(shape, width):
    return lax.broadcasted_iota(jnp.int32, shape, 1) // width


def pick_groups(groups, parts):
    value = parts[-1]
    for number in range(len(parts) - 2, -1, -1):
        value = jnp.where(groups == number, parts[number], value)
    return value


def toeplitz(rows):
    tiles = []
    for j in range(8):
        halves = []
        for half in range(2):
            spread = jnp.broadcast_to(rows[2 * j + half : 2 * j + half + 1], (GROUP, LANES))
            halves.append(pltpu.roll(spread, 0, 1, stride=1, stride_axis=0))
        tiles.append(jnp.concatenate(halves, axis=1))
    return jnp.concatenate(tiles, axis=0).astype(jnp.bfloat16)


def blur(left, right, matrix):
    groups = lane_group(left.shape, GROUP)
    low = groups < 2
    by32, by64, by96 = turn(left, 32, 1), turn(left, 64, 1), turn(left, 96, 1)
    end32, end96 = turn(right, 32, 1), turn(right, 96, 1)
    framed = [
        jnp.where(low, left, by64),
        jnp.where(low, by96, by32),
        jnp.where(low, by64, left),
        pick_groups(groups, [by32, end32, by96, end96]),
    ]
    summed = []
    for part in framed:
        first = jnp.where(low, part, turn(part, -1, 0))
        stacked = jnp.concatenate([first, turn(first, -2, 0)], axis=1).astype(jnp.bfloat16)
        product = lax.dot_general(
            stacked, matrix, (((1,), (1,)), ((), ())), preferred_element_type=jnp.float32
        )
        joined = product[:, :LANES] + turn(product[:, LANES:], -16, 0)
        summed.append(pick_groups(groups, [turn(joined, -4 * j, 0) for j in range(4)]))
    total = pick_groups(groups, summed)
    for step in range(1, 4):
        chosen = pick_groups(groups, [summed[(j + step) % 4] for j in range(4)])
        total = total + turn(chosen, 32 * step, 1)
    return total


def blur_back(image, matrix):
    groups = lane_group(image.shape, GROUP)
    low = groups < 2
    turned = [turn(image, 32 * step, 1) for step in range(4)]
    folded = []
    for h in range(4):
        spread = pick_groups(groups, [turned[(j - h) % 4] for j in range(4)])
        first = pick_groups(groups, [turn(spread, 4 * j, 0) for j in range(4)])
        stacked = jnp.concatenate([first, turn(first, 16, 0)], axis=1).astype(jnp.bfloat16)
        product = jnp.dot(stacked, matrix, preferred_element_type=jnp.float32)
        joined = product[:, :LANES] + turn(product[:, LANES:], 2, 0)
        shifted = jnp.where(low, joined, turn(joined, 1, 0))
        folded.append(shifted + turn(shifted, 64, 1))
    one, three = turn(folded[1], 32, 1), turn(folded[3], 32, 1)
    zero = jnp.zeros_like(one)
    left = jnp.where(low, folded[0], folded[2]) + pick_groups(groups, [zero, one, one, three])
    right = jnp.where(groups == 0, three, 0.0)
    return left, right


def place(total_ref, cell, per_row, block, patch):
    left, right = patch
    rows = pl.ds(pl.multiple_of(cell // per_row * block, block), left.shape[0])
    start = pl.multiple_of(cell % per_row * block, block)
    total_ref[rows, pl.ds(start, block)] += left
    total_ref[rows, pl.ds(pl.multiple_of(start + block, block), block)] += right


def pack_kernel(count, source_ref, tag_ref, exposures_ref, taps_ref, out_ref):
    block = exposures_ref.shape[1]

    @pl.loop(0, count)
    def _(slot):
        origin = source_ref[slot]
        out_ref[slot, :block, :] = exposures_ref[origin].astype(jnp.bfloat16)
        out_ref[slot, block : block + 16, :] = taps_ref[origin]
        out_ref[slot, block + 16 :, :] = jnp.full((16, LANES), tag_ref[slot], jnp.float32).astype(
            jnp.bfloat16
        )


def first_kernel(count, per_row, block, cell_ref, frames_ref, total_ref, matrix_ref):
    total_ref[...] = jnp.zeros_like(total_ref)

    @pl.loop(0, count)
    def _(slot):
        cell = cell_ref[slot]

        @pl.when(cell >= 0)
        def _():
            frame = frames_ref[slot]
            matrix = toeplitz(frame[block : block + 16].astype(jnp.float32))
            matrix_ref[slot] = matrix
            image = frame[:block].astype(jnp.float32)
            image = jnp.concatenate([image, jnp.zeros((GROUP, LANES), jnp.float32)], axis=0)
            place(total_ref, cell, per_row, block, blur_back(image, matrix))


def normal_kernel(count, per_row, block, cell_ref, field_ref, matrix_ref, total_ref):
    total_ref[...] = jnp.zeros_like(total_ref)
    window = block + GROUP

    @pl.loop(0, count)
    def _(slot):
        cell = cell_ref[slot]

        @pl.when(cell >= 0)
        def _():
            matrix = matrix_ref[slot]
            rows = pl.ds(pl.multiple_of(cell // per_row * block, block), window)
            start = pl.multiple_of(cell % per_row * block, block)
            left = field_ref[rows, pl.ds(start, block)].astype(jnp.float32)
            right = field_ref[rows, pl.ds(pl.multiple_of(start + block, block), block)].astype(
                jnp.float32
            )
            modelled = blur(left, right, matrix).astype(jnp.bfloat16).astype(jnp.float32)
            inside = lax.broadcasted_iota(jnp.int32, modelled.shape, 0) < block
            image = jnp.where(inside, modelled, 0.0)
            place(total_ref, cell, per_row, block, blur_back(image, matrix))


def sum_kernel(axes, own_ref, out_ref, *scratch):
    barrier = pltpu.get_barrier_semaphore()
    peers = 0
    for axis, size in axes:
        me = lax.axis_index(axis)
        for step in range(1, size):
            pl.semaphore_signal(
                barrier,
                inc=1,
                device_id={axis: lax.rem(me + step, size)},
                device_id_type=pl.DeviceIdType.MESH,
            )
        peers += size - 1
    pl.semaphore_wait(barrier, peers)
    source = own_ref
    for number, (axis, size) in enumerate(axes):
        total_ref, landed, sent, received = scratch[4 * number : 4 * number + 4]
        me = lax.axis_index(axis)
        copies = [
            pltpu.make_async_remote_copy(
                src_ref=source,
                dst_ref=landed.at[step - 1],
                send_sem=sent.at[step - 1],
                recv_sem=received.at[step - 1],
                device_id={axis: lax.rem(me + step, size)},
                device_id_type=pl.DeviceIdType.MESH,
            )
            for step in range(1, size)
        ]
        for copy in copies:
            copy.start()
        for copy in copies:
            copy.wait()
        total = source[...]
        for step in range(size - 1):
            total = total + landed[step]
        total_ref[...] = total
        source = total_ref
    out_ref[...] = source[...]


def sum_over_mesh(values, number):
    axes = [(axis, lax.axis_size(axis)) for axis in ("ty", "tx")]
    shape = (8, LANES)
    scratch = []
    for _, size in axes:
        scratch += [
            pltpu.VMEM(shape, jnp.float32),
            pltpu.VMEM((size - 1,) + shape, jnp.float32),
            pltpu.SemaphoreType.DMA((size - 1,)),
            pltpu.SemaphoreType.DMA((size - 1,)),
        ]
    rows = jnp.pad(values, (0, shape[0] - values.shape[0]))
    summed = pl.pallas_call(
        functools.partial(sum_kernel, axes),
        out_shape=jax.ShapeDtypeStruct(shape, jnp.float32),
        in_specs=[vmem()],
        out_specs=vmem(),
        scratch_shapes=scratch,
        compiler_params=pltpu.CompilerParams(collective_id=number, has_side_effects=True),
        name="sum_mesh",
    )(jnp.broadcast_to(rows[:, None], shape))
    return [summed[row, 0] for row in range(values.shape[0])]


def vmem():
    return pl.BlockSpec(memory_space=pltpu.VMEM)


def smem():
    return pl.BlockSpec(memory_space=pltpu.SMEM)


def flat_strip(strip):
    count = LANES // strip.shape[1]
    parts = strip.reshape(count, strip.shape[0] // count, strip.shape[1])
    return jnp.concatenate([parts[i] for i in range(count)], axis=1)


def tall_strip(flat, shape):
    count = LANES // shape[1]
    return jnp.concatenate([flat[:, i * shape[1] : (i + 1) * shape[1]] for i in range(count)], axis=0)


def share_edges(value, axis, dim, width):
    size, length = lax.axis_size(axis), value.shape[dim]
    position = lax.axis_index(axis)
    up = [(i, i + 1) for i in range(size - 1)]
    down = [(j, i) for i, j in up]
    first = lax.slice_in_dim(value, 0, 2 * width, axis=dim)
    middle = lax.slice_in_dim(value, 2 * width, length - 2 * width, axis=dim)
    last = lax.slice_in_dim(value, length - 2 * width, length, axis=dim)
    if dim == 1:
        before = lax.ppermute(flat_strip(last), axis, up)
        after = lax.ppermute(flat_strip(first), axis, down)
        before, after = tall_strip(before, last.shape), tall_strip(after, first.shape)
    else:
        before = lax.ppermute(last, axis, up)
        after = lax.ppermute(first, axis, down)
    index = lax.broadcasted_iota(jnp.int32, first.shape, dim)
    first = jnp.where((position > 0) | (index >= width), first + before, 0.0)
    last = jnp.where((position < size - 1) | (index < width), last + after, 0.0)
    return jnp.concatenate([first, middle, last], axis=dim)


def body(exposures, point_spread, warp_steps, column, block_cell):
    frame_count, block = exposures.shape[:2]
    tap_count = point_spread.shape[1] + 1
    margin = tap_count // 2
    tx_size = lax.axis_size("tx")
    capacity = max(2, 2 * frame_count // tx_size)
    slot_count = tx_size * capacity
    per_row = TILE // block
    extent = TILE + 2 * margin
    wide = TILE + block
    taps = make_kernels(point_spread, warp_steps)
    taps = jnp.pad(taps, ((0, 0), (0, 0), (0, 64 - tap_count))).reshape(frame_count, 16, LANES)

    target = column[:, 0]
    earlier = jnp.arange(frame_count)[:, None] > jnp.arange(frame_count)[None, :]
    matching = target[:, None] == target[None, :]
    standing = jnp.sum(jnp.where(earlier & matching, 1, 0), axis=1)
    slot_index = target * capacity + standing
    chosen = slot_index[None, :] == jnp.arange(slot_count)[:, None]
    source = jnp.sum(jnp.where(chosen, jnp.arange(frame_count)[None, :], 0), axis=1).astype(jnp.int32)
    tag = jnp.sum(jnp.where(chosen, block_cell[None, :] + 1, 0), axis=1).astype(jnp.float32)

    packed = pl.pallas_call(
        functools.partial(pack_kernel, slot_count),
        out_shape=jax.ShapeDtypeStruct((slot_count, block + 32, LANES), jnp.bfloat16),
        in_specs=[smem(), smem(), vmem(), vmem()],
        out_specs=vmem(),
        name="pack",
    )(source, tag, exposures, taps)
    frames = lax.all_to_all(packed, "tx", split_axis=0, concat_axis=0, tiled=True)
    cells = frames[:, block + 16, 0].astype(jnp.int32) - 1

    total, matrices = pl.pallas_call(
        functools.partial(first_kernel, slot_count, per_row, block),
        out_shape=(
            jax.ShapeDtypeStruct((extent, wide), jnp.float32),
            jax.ShapeDtypeStruct((slot_count, 256, 256), jnp.bfloat16),
        ),
        in_specs=[smem(), vmem()],
        out_specs=(vmem(), vmem()),
        name="first_adjoint",
    )(cells, frames)

    def finish(total):
        value = share_edges(total[:, :extent], "ty", 0, margin)
        return share_edges(value, "tx", 1, margin)

    def inner(value):
        return value[margin : margin + TILE, margin : margin + TILE]

    def products(pairs):
        return tuple(jnp.sum(inner(left * right)) for left, right in pairs)

    residual = finish(total)
    direction = residual
    solution = jnp.zeros((TILE, TILE), jnp.float32)
    norm_now = None
    for iteration in range(ITERS):
        field = jnp.pad(direction.astype(jnp.bfloat16), ((0, 0), (0, wide - extent)))
        total = pl.pallas_call(
            functools.partial(normal_kernel, slot_count, per_row, block),
            out_shape=jax.ShapeDtypeStruct((extent, wide), jnp.float32),
            in_specs=[smem(), vmem(), vmem()],
            out_specs=vmem(),
            name="normal",
        )(cells, field, matrices)
        applied = finish(total) + damping * direction
        last = iteration + 1 == ITERS
        pairs = [(direction, applied)]
        if not last:
            pairs = pairs + [(residual, applied), (applied, applied)]
        if norm_now is None:
            pairs = pairs + [(residual, residual)]
        sums = sum_over_mesh(jnp.stack(products(pairs)), iteration)
        if norm_now is None:
            norm_now = sums[-1]
        step_size = norm_now / sums[0]
        solution = solution + step_size * inner(direction)
        residual = residual - step_size * applied
        if not last:
            norm_next = norm_now - 2.0 * step_size * sums[1] + step_size * step_size * sums[2]
            direction = residual + norm_next / norm_now * direction
            norm_now = norm_next
    return solution, inner(residual)


def solution(mesh):
    placed = (
        P(("ty", "tx"), None, None),
        P(("ty", "tx"), None, None),
        P(("ty", "tx"), None),
        P(("ty", "tx"), None),
        P(("ty", "tx")),
    )
    return jax.shard_map(
        body, mesh=mesh, in_specs=placed, out_specs=(P("ty", "tx"), P("ty", "tx")), check_vma=False
    )
```
